16 devices in a mesh: dp: 2 (over y, z), tp: 8 (over x, core).
Axes of the slice: x: 4, y: 2, z: 1, core: 2. Of those that a mesh axis runs over, the one named last changes fastest.
The devices are a block of a 4x4x8 slice.
Arguments:
- query: bfloat16 [128, 32, 128], P('dp', 'tp'), parts along dimension 0
- k_cache: bfloat16 [128, 1024, 8, 128], P('dp', None, 'tp'), parts along dimension 0
- v_cache: bfloat16 [128, 1024, 8, 128], P('dp', None, 'tp'), parts along dimension 0
- k_new: bfloat16 [128, 8, 128], P('dp', 'tp'), parts along dimension 0
- v_new: bfloat16 [128, 8, 128], P('dp', 'tp'), parts along dimension 0
- lens: int32 [128], P('dp'), parts along dimension 0
Outputs:
- output 1: bfloat16 [128, 32, 128], P('dp', 'tp'), parts along dimension 0
- output 2: bfloat16 [128, 1024, 8, 128], P('dp', 'tp'), parts along dimension 0
- output 3: bfloat16 [128, 1024, 8, 128], P('dp', 'tp'), parts along dimension 0
There are 2 independent parts. The reference program is written for one: setup_inputs(seed, part) draws one part's arguments, and reference() takes and returns one part's arrays. A program takes and returns all parts, laid end to end along the dimension named above; each array names one.
All inputs are finite; a program needn't handle non-finite values.
Results may differ from the reference program's by a relative error of at most 0.00772032.
Values are sent between devices in bfloat16 or wider.
A program may use at most 768 MiB of HBM per device.

```python
import math
import jax
import jax.numpy as jnp
from jax import lax

BATCH = 64
SEQ_LEN = 1024
Q_HEADS = 32
KV_HEADS = 8
HEAD_DIM = 128


def setup_inputs(seed: int = 0, part: int = 0) -> dict:
    base_key = jax.random.fold_in(jax.random.key(seed), part)
    keys = jax.random.split(base_key, 6)
    group_size = Q_HEADS // KV_HEADS
    spread = math.sqrt(math.log(SEQ_LEN))
    align = 1.4 * math.sqrt(math.log(SEQ_LEN) / HEAD_DIM)
    cache_shape = (BATCH, SEQ_LEN, KV_HEADS, HEAD_DIM)
    k_cache = jax.random.normal(keys[0], cache_shape, jnp.float32)
    v_cache = jax.random.normal(keys[1], cache_shape, jnp.float32)
    k_new = jax.random.normal(keys[2], (BATCH, KV_HEADS, HEAD_DIM), jnp.float32)
    v_new = jax.random.normal(keys[3], (BATCH, KV_HEADS, HEAD_DIM), jnp.float32)
    noise = jax.random.normal(keys[4], (BATCH, KV_HEADS, group_size, HEAD_DIM), jnp.float32)
    mixed = math.sqrt(1.0 - align * align) * noise + align * k_new[:, :, None, :]
    query = (spread * mixed).reshape(BATCH, Q_HEADS, HEAD_DIM)
    len_keys = jax.random.split(keys[5])
    low_len = SEQ_LEN // 8
    lens = jax.random.randint(len_keys[0], (BATCH,), low_len, SEQ_LEN, jnp.int32)
    top_slot = jax.random.randint(len_keys[1], (), 0, BATCH, jnp.int32)
    lens = jnp.where(jnp.arange(BATCH) == top_slot, SEQ_LEN - 1, lens)
    return {"query": query.astype(jnp.bfloat16), "k_cache": k_cache.astype(jnp.bfloat16), "v_cache": v_cache.astype(jnp.bfloat16), "k_new": k_new.astype(jnp.bfloat16), "v_new": v_new.astype(jnp.bfloat16), "lens": lens}


def reference(query, k_cache, v_cache, k_new, v_new, lens):
    positions = jnp.arange(SEQ_LEN, dtype=jnp.int32)
    new_slot = (positions[None, :] == lens[:, None])[:, :, None, None]
    k_upd = jnp.where(new_slot, k_new[:, None], k_cache)
    v_upd = jnp.where(new_slot, v_new[:, None], v_cache)
    group_size = Q_HEADS // KV_HEADS
    inv_sqrt = HEAD_DIM ** -0.5

    def one_head(head_in):
        q_head, k_head, v_head, length = head_in
        scores = jnp.dot(q_head, k_head.T, preferred_element_type=jnp.float32) * inv_sqrt
        scores = jnp.where(positions[None, :] <= length, scores, -1e30)
        probs = jax.nn.softmax(scores, axis=-1)
        return jnp.dot(probs.astype(jnp.bfloat16), v_head, preferred_element_type=jnp.float32)

    q_flat = query.reshape(BATCH * KV_HEADS, group_size, HEAD_DIM)
    k_flat = jnp.swapaxes(k_upd, 1, 2).reshape(BATCH * KV_HEADS, SEQ_LEN, HEAD_DIM)
    v_flat = jnp.swapaxes(v_upd, 1, 2).reshape(BATCH * KV_HEADS, SEQ_LEN, HEAD_DIM)
    len_flat = jnp.repeat(lens, KV_HEADS)
    head_out = lax.map(one_head, (q_flat, k_flat, v_flat, len_flat))
    attn_out = head_out.reshape(BATCH, Q_HEADS, HEAD_DIM).astype(jnp.bfloat16)
    return attn_out, k_upd, v_upd
```

```python
import functools

import jax
import jax.numpy as jnp
from jax import lax
from jax.experimental import pallas as pl
from jax.experimental.pallas import tpu as pltpu
from jax.sharding import PartitionSpec as P

MESH = pl.DeviceIdType.MESH
MASK_VALUE = -1e30


def exchange_kernel(n, q_ref, k_ref, v_ref, kn_ref, vn_ref, lens_ref,
                    out_ref, kx_ref, vx_ref, knx_ref, vnx_ref,
                    kbuf, vbuf, kn32, vn32, send_sem, recv_sem, small_send, small_recv, load_sem, keep_sem):
    dp, me = lax.axis_index("dp"), lax.axis_index("tp")
    batch, seq_len, head_dim = k_ref.shape
    seq_local = seq_len // n

    barrier = pltpu.get_barrier_semaphore()
    for step in range(1, n):
        pl.semaphore_signal(barrier, inc=1, device_id=(dp, lax.rem(me + step, n)), device_id_type=MESH)
    pl.semaphore_wait(barrier, n - 1)

    def rows(peer):
        return pl.ds(pl.multiple_of(peer * seq_local, seq_local), seq_local)

    copies = []
    for a, (src, dst) in enumerate(((k_ref, kx_ref), (v_ref, vx_ref))):
        for slot, step in enumerate(STEPS):
            peer = lax.rem(me + step, n)
            copy = pltpu.make_async_remote_copy(
                src_ref=src.at[:, rows(peer)], dst_ref=dst.at[me],
                send_sem=send_sem.at[a, slot], recv_sem=recv_sem.at[a, slot],
                device_id=(dp, peer), device_id_type=MESH)
            copy.start()
            copies.append(copy)
    for a, (src, dst) in enumerate(((kn_ref, knx_ref), (vn_ref, vnx_ref))):
        for slot, step in enumerate(STEPS):
            copy = pltpu.make_async_remote_copy(
                src_ref=src, dst_ref=dst.at[me],
                send_sem=small_send.at[a, slot], recv_sem=small_recv.at[a, slot],
                device_id=(dp, lax.rem(me + step, n)), device_id_type=MESH)
            copy.start()
            copies.append(copy)
    own_new = [pltpu.make_async_copy(kn_ref, knx_ref.at[me], keep_sem.at[0, 2]),
               pltpu.make_async_copy(vn_ref, vnx_ref.at[me], keep_sem.at[1, 2])]
    for copy in own_new:
        copy.start()

    kn32[...] = kn_ref[...].astype(jnp.float32)
    vn32[...] = vn_ref[...].astype(jnp.float32)

    def load(a, b, slot):
        src, dst = ((k_ref, kbuf), (v_ref, vbuf))[a]
        return pltpu.make_async_copy(src.at[b], dst.at[slot], load_sem.at[a, slot])

    def keep(a, b, slot):
        src, dst = ((kbuf, kx_ref), (vbuf, vx_ref))[a]
        return pltpu.make_async_copy(src.at[slot, rows(me)], dst.at[me, b], keep_sem.at[a, slot])

    for a in range(2):
        load(a, 0, 0).start()
    scale = head_dim ** -0.5
    positions = lax.broadcasted_iota(jnp.int32, (1, seq_len), 1)

    def attend(b, carry):
        slot = lax.rem(b, 2)
        for a in range(2):
            load(a, b, slot).wait()
            keep(a, b, slot).start()

        @pl.when(b > 0)
        def _():
            for a in range(2):
                keep(a, b - 1, 1 - slot).wait()

        @pl.when(b + 1 < batch)
        def _():
            for a in range(2):
                load(a, b + 1, 1 - slot).start()

        length = lens_ref[b]
        query = q_ref[b]
        new_k, new_v = kn32[pl.ds(b, 1), :], vn32[pl.ds(b, 1), :]
        scores = lax.dot_general(query, kbuf[slot], (((1,), (1,)), ((), ())), preferred_element_type=jnp.float32)
        new_score = jnp.sum(query.astype(jnp.float32) * new_k, axis=-1, keepdims=True)
        is_new = positions == length
        scores = jnp.where(is_new, new_score, scores) * scale
        scores = jnp.where(positions <= length, scores, MASK_VALUE)
        weights = jnp.exp(scores - jnp.max(scores, axis=-1, keepdims=True))
        weights = weights / jnp.sum(weights, axis=-1, keepdims=True)
        probs = weights.astype(jnp.bfloat16)
        old = jnp.where(is_new, 0.0, weights).astype(jnp.bfloat16)
        summed = jnp.dot(old, vbuf[slot], preferred_element_type=jnp.float32)
        new_prob = jnp.sum(jnp.where(is_new, probs.astype(jnp.float32), 0.0), axis=-1, keepdims=True)
        out_ref[b] = (summed + new_prob * new_v).astype(jnp.bfloat16)
        return carry

    lax.fori_loop(0, batch, attend, 0)
    for a in range(2):
        keep(a, batch - 1, (batch - 1) % 2).wait()
    for copy in own_new:
        copy.wait()
    for copy in copies:
        copy.wait()


STEPS = (4, 5, 3, 2, 6, 1, 7)


def relayout_kernel(n, lens_ref, kx_ref, vx_ref, knx_ref, vnx_ref, ko_ref, vo_ref, wide, kn32, vn32):
    block, seq_local = ko_ref.shape[0], ko_ref.shape[1]
    batch = knx_ref.shape[1]
    step = pl.program_id(0)
    base = lax.axis_index("tp") * seq_local

    @pl.when(step == 0)
    def _():
        for h in range(n):
            kn32[pl.ds(h, batch, stride=n), :] = knx_ref[h].astype(jnp.float32)
            vn32[pl.ds(h, batch, stride=n), :] = vnx_ref[h].astype(jnp.float32)

    for a, (src, dst, new) in enumerate(((kx_ref, ko_ref, kn32), (vx_ref, vo_ref, vn32))):
        for i in range(block):
            s = (a * block + i) % 2
            for h in range(n):
                wide[s, pl.ds(h, seq_local, stride=n), :] = src[h, i].astype(jnp.float32)
            dst[i] = wide[s].reshape(seq_local, n, -1).astype(jnp.bfloat16)
            b = step * block + i
            row = lens_ref[b] - base

            @pl.when((row >= 0) & (row < seq_local))
            def _():
                dst[i, row] = new[pl.ds(pl.multiple_of(b * n, n), n), :].astype(jnp.bfloat16)


def solution(mesh):
    n = mesh.shape["tp"]

    def local_step(query, k_cache, v_cache, k_new, v_new, lens):
        batch, seq_len, _, head_dim = k_cache.shape
        seq_local = seq_len // n
        k_cache = k_cache.reshape(batch, seq_len, head_dim)
        v_cache = v_cache.reshape(batch, seq_len, head_dim)
        k_new = k_new.reshape(batch, head_dim)
        v_new = v_new.reshape(batch, head_dim)
        dtype = k_cache.dtype
        any_spec = pl.BlockSpec(memory_space=pl.ANY)
        vmem_spec = pl.BlockSpec(memory_space=pltpu.VMEM)
        smem_spec = pl.BlockSpec(memory_space=pltpu.SMEM)
        held = jax.ShapeDtypeStruct((n, batch, seq_local, head_dim), dtype)
        held_new = jax.ShapeDtypeStruct((n, batch, head_dim), dtype)
        attn_out, kx, vx, knx, vnx = pl.pallas_call(
            functools.partial(exchange_kernel, n),
            name="exchange_attend",
            out_shape=[jax.ShapeDtypeStruct(query.shape, dtype), held, held, held_new, held_new],
            in_specs=[vmem_spec, any_spec, any_spec, vmem_spec, vmem_spec, smem_spec],
            out_specs=[vmem_spec, any_spec, any_spec, any_spec, any_spec],
            scratch_shapes=[
                pltpu.VMEM((2, seq_len, head_dim), dtype),
                pltpu.VMEM((2, seq_len, head_dim), dtype),
                pltpu.VMEM((batch, head_dim), jnp.float32),
                pltpu.VMEM((batch, head_dim), jnp.float32),
                pltpu.SemaphoreType.DMA((2, n - 1)),
                pltpu.SemaphoreType.DMA((2, n - 1)),
                pltpu.SemaphoreType.DMA((2, n - 1)),
                pltpu.SemaphoreType.DMA((2, n - 1)),
                pltpu.SemaphoreType.DMA((2, 2)),
                pltpu.SemaphoreType.DMA((2, 3)),
            ],
            compiler_params=pltpu.CompilerParams(collective_id=0, has_side_effects=True),
        )(query, k_cache, v_cache, k_new, v_new, lens)

        block = 2
        moved = jax.ShapeDtypeStruct((batch, seq_local, n, head_dim), dtype)
        in_block = pl.BlockSpec((n, block, seq_local, head_dim), lambda i: (0, i, 0, 0))
        out_block = pl.BlockSpec((block, seq_local, n, head_dim), lambda i: (i, 0, 0, 0))
        new_block = pl.BlockSpec((n, batch, head_dim), lambda i: (0, 0, 0))
        k_out, v_out = pl.pallas_call(
            functools.partial(relayout_kernel, n),
            name="relayout",
            grid=(batch // block,),
            out_shape=[moved, moved],
            in_specs=[smem_spec, in_block, in_block, new_block, new_block],
            out_specs=[out_block, out_block],
            scratch_shapes=[
                pltpu.VMEM((2, seq_local * n, head_dim), jnp.float32),
                pltpu.VMEM((batch * n, head_dim), jnp.float32),
                pltpu.VMEM((batch * n, head_dim), jnp.float32),
            ],
        )(lens, kx, vx, knx, vnx)
        return attn_out, k_out, v_out

    head_spec = P("dp", "tp")
    entry_spec = P("dp", None, "tp")
    return jax.shard_map(local_step, mesh=mesh, in_specs=(head_spec, entry_spec, entry_spec, head_spec, head_spec, P("dp")), out_specs=(head_spec, P("dp", "tp"), P("dp", "tp")), check_vma=False)
```

```python
import functools

import jax
import jax.numpy as jnp
from jax import lax
from jax.experimental import pallas as pl
from jax.experimental.pallas import tpu as pltpu
from jax.sharding import PartitionSpec as P

MESH = pl.DeviceIdType.MESH
MASK_VALUE = -1e30
TAIL = 8


def exchange_kernel(n, q_hbm, k_ref, v_ref, kn_hbm, vn_hbm, lens_ref,
                    out_hbm, kx_ref, vx_ref, knx_ref, vnx_ref, vt_ref,
                    kbuf, vbuf, q_ref, out_ref, kn_ref, vn_ref, kn32, vn32,
                    send_sem, recv_sem, small_send, small_recv, load_sem, keep_sem, tail_sem, once_sem):
    dp, me = lax.axis_index("dp"), lax.axis_index("tp")
    batch, seq_len, head_dim = k_ref.shape
    seq_local = seq_len // n
    head_part = vx_ref.shape[1]
    chips = n // 2
    chip = me // 2
    core = me - 2 * chip

    def at(hops, other):
        return 2 * lax.rem(chip + hops, chips) + (1 - core if other else core)

    sibling = at(0, True)
    far = chips // 2
    near = [h for h in range(1, chips) if h != far]
    targets = [at(far, False), at(far, True)] + [at(h, False) for h in near] + [at(h, True) for h in near] + [sibling]

    barrier = pltpu.get_barrier_semaphore()
    for step in range(1, n):
        pl.semaphore_signal(barrier, inc=1, device_id=(dp, lax.rem(me + step, n)), device_id_type=MESH)
    pl.semaphore_wait(barrier, n - 1)

    def rows(peer):
        return pl.ds(pl.multiple_of(peer * seq_local, seq_local), seq_local)

    def remote(src, dst, send, recv, peer):
        return pltpu.make_async_remote_copy(src_ref=src, dst_ref=dst, send_sem=send, recv_sem=recv,
                                            device_id=(dp, peer), device_id_type=MESH)

    copies = []
    for a, (src, dst) in enumerate(((kn_hbm, knx_ref), (vn_hbm, vnx_ref))):
        for h in range(1, chips):
            copies.append(remote(src, dst.at[me], small_send.at[a, h], small_recv.at[a, h], at(h, False)))
        copies.append(remote(src, dst.at[me], small_send.at[a, 0], small_recv.at[a, 0], sibling))
    for a, (src, dst) in enumerate(((k_ref, kx_ref), (v_ref, vx_ref))):
        for slot, peer in enumerate(targets):
            copies.append(remote(src.at[pl.ds(0, dst.shape[1]), rows(peer)], dst.at[me],
                                 send_sem.at[a, slot], recv_sem.at[a, slot], peer))
    for copy in copies:
        copy.start()

    def load(a, b, slot):
        src, dst = ((k_ref, kbuf), (v_ref, vbuf))[a]
        return pltpu.make_async_copy(src.at[b], dst.at[slot], load_sem.at[a, slot])

    first = [pltpu.make_async_copy(kn_hbm, kn_ref, once_sem.at[0]),
             pltpu.make_async_copy(vn_hbm, vn_ref, once_sem.at[1]),
             pltpu.make_async_copy(q_hbm, q_ref, once_sem.at[2])]
    for copy in first:
        copy.start()
    for a in range(2):
        load(a, 0, 0).start()
    for copy in first:
        copy.wait()
    own_new = [pltpu.make_async_copy(kn_ref, knx_ref.at[me], once_sem.at[0]),
               pltpu.make_async_copy(vn_ref, vnx_ref.at[me], once_sem.at[1])]
    tail = [pltpu.make_async_copy(v_ref.at[pl.ds(head_part, batch - head_part), pl.ds(p * seq_local, seq_local)],
                                  vt_ref.at[p], tail_sem.at[p]) for p in range(n)]
    for copy in own_new + tail:
        copy.start()
    kn32[...] = kn_ref[...].astype(jnp.float32)
    vn32[...] = vn_ref[...].astype(jnp.float32)

    def keep(b, slot, act):
        act(pltpu.make_async_copy(kbuf.at[slot, rows(me)], kx_ref.at[me, b], keep_sem.at[0, slot]))

        @pl.when(b < head_part)
        def _():
            act(pltpu.make_async_copy(vbuf.at[slot, rows(me)], vx_ref.at[me, b], keep_sem.at[1, slot]))

    scale = head_dim ** -0.5
    positions = lax.broadcasted_iota(jnp.int32, (1, seq_len), 1)

    def attend(b, carry):
        slot = lax.rem(b, 2)
        for a in range(2):
            load(a, b, slot).wait()
        keep(b, slot, lambda copy: copy.start())

        @pl.when(b > 0)
        def _():
            keep(b - 1, 1 - slot, lambda copy: copy.wait())

        @pl.when(b + 1 < batch)
        def _():
            for a in range(2):
                load(a, b + 1, 1 - slot).start()

        length = lens_ref[b]
        query = q_ref[b]
        new_k, new_v = kn32[pl.ds(b, 1), :], vn32[pl.ds(b, 1), :]
        scores = lax.dot_general(query, kbuf[slot], (((1,), (1,)), ((), ())), preferred_element_type=jnp.float32)
        new_score = jnp.sum(query.astype(jnp.float32) * new_k, axis=-1, keepdims=True)
        is_new = positions == length
        scores = jnp.where(is_new, new_score, scores) * scale
        scores = jnp.where(positions <= length, scores, MASK_VALUE)
        weights = jnp.exp(scores - jnp.max(scores, axis=-1, keepdims=True))
        weights = weights / jnp.sum(weights, axis=-1, keepdims=True)
        probs = weights.astype(jnp.bfloat16)
        old = jnp.where(is_new, 0.0, weights).astype(jnp.bfloat16)
        summed = jnp.dot(old, vbuf[slot], preferred_element_type=jnp.float32)
        new_prob = jnp.sum(jnp.where(is_new, probs.astype(jnp.float32), 0.0), axis=-1, keepdims=True)
        out_ref[b] = (summed + new_prob * new_v).astype(jnp.bfloat16)
        return carry

    lax.fori_loop(0, batch, attend, 0)
    keep(batch - 1, (batch - 1) % 2, lambda copy: copy.wait())
    for copy in own_new + tail:
        copy.wait()
    done = pltpu.make_async_copy(out_ref, out_hbm, once_sem.at[2])
    done.start()

    passed = []
    for a, dst in enumerate((knx_ref, vnx_ref)):
        for h in range(1, chips):
            origin = at(chips - h, False)
            remote(dst.at[me], dst.at[me], small_send.at[a, h], small_recv.at[a, h], at(h, False)).wait_recv()
            passed.append(remote(dst.at[origin], dst.at[origin], small_send.at[a, chips + h], small_recv.at[a, chips + h], sibling))
            passed[-1].start()
    for i, copy in enumerate(copies):
        copy.wait_send()
        if not any(i in range(a * chips, a * chips + chips - 1) for a in range(2)):
            copy.wait_recv()
    for copy in passed:
        copy.wait()
    done.wait()


def new_rows(n, new_ref, new32):
    for h in range(n):
        new32[pl.ds(h, new_ref.shape[1], stride=n), :] = new_ref[h].astype(jnp.float32)


def place(n, x_ref, i, o_ref, j, row, b, new32):
    o_ref[j] = jnp.swapaxes(x_ref[:, i], 0, 1)

    @pl.when((row >= 0) & (row < o_ref.shape[1]))
    def _():
        o_ref[j, row] = new32[pl.ds(pl.multiple_of(b * n, n), n), :].astype(o_ref.dtype)


def relayout_kernel(n, lens_ref, out_in, kx_ref, vx_ref, knx_ref, vnx_ref, out_ref, ko_ref, vo_ref, kn32, vn32):
    step = pl.program_id(0)
    base = lax.axis_index("tp") * ko_ref.shape[1]

    @pl.when(step == 0)
    def _():
        out_ref[...] = out_in[...]
        new_rows(n, knx_ref, kn32)
        new_rows(n, vnx_ref, vn32)

    for x_ref, o_ref, new32 in ((kx_ref, ko_ref, kn32), (vx_ref, vo_ref, vn32)):
        block = o_ref.shape[0]
        for i in range(block):
            b = step * block + i
            place(n, x_ref, i, o_ref, i, lens_ref[b] - base, b, new32)


def tail_kernel(n, first, lens_ref, x_ref, new_ref, whole_ref, o_ref, new32):
    step = pl.program_id(0)
    block = o_ref.shape[0]
    base = lax.axis_index("tp") * o_ref.shape[1]

    @pl.when(step == 0)
    def _():
        new_rows(n, new_ref, new32)

    for i in range(block):
        b = first + step * block + i
        place(n, x_ref, step * block + i, o_ref, i, lens_ref[b] - base, b, new32)


def solution(mesh):
    n = mesh.shape["tp"]

    def local_step(query, k_cache, v_cache, k_new, v_new, lens):
        batch, seq_len, _, head_dim = k_cache.shape
        seq_local = seq_len // n
        k_cache = k_cache.reshape(batch, seq_len, head_dim)
        v_cache = v_cache.reshape(batch, seq_len, head_dim)
        k_new = k_new.reshape(batch, head_dim)
        v_new = v_new.reshape(batch, head_dim)
        dtype = k_cache.dtype
        any_spec = pl.BlockSpec(memory_space=pl.ANY)
        vmem_spec = pl.BlockSpec(memory_space=pltpu.VMEM)
        smem_spec = pl.BlockSpec(memory_space=pltpu.SMEM)
        held = lambda count: jax.ShapeDtypeStruct((n, count, seq_local, head_dim), dtype)
        held_new = jax.ShapeDtypeStruct((n, batch, head_dim), dtype)
        head_shape = jax.ShapeDtypeStruct(query.shape, dtype)
        dma = lambda *shape: pltpu.SemaphoreType.DMA(shape)
        attn, kx, vx, knx, vnx, vt = pl.pallas_call(
            functools.partial(exchange_kernel, n),
            name="exchange_attend",
            out_shape=[head_shape, held(batch), held(batch - TAIL), held_new, held_new, held(TAIL)],
            in_specs=[any_spec] * 5 + [smem_spec],
            out_specs=[any_spec] * 6,
            scratch_shapes=[
                pltpu.VMEM((2, seq_len, head_dim), dtype),
                pltpu.VMEM((2, seq_len, head_dim), dtype),
                pltpu.VMEM(query.shape, dtype),
                pltpu.VMEM(query.shape, dtype),
                pltpu.VMEM((batch, head_dim), dtype),
                pltpu.VMEM((batch, head_dim), dtype),
                pltpu.VMEM((batch, head_dim), jnp.float32),
                pltpu.VMEM((batch, head_dim), jnp.float32),
                dma(2, n - 1), dma(2, n - 1), dma(2, n), dma(2, n), dma(2, 2), dma(2, 2), dma(n), dma(3),
            ],
            compiler_params=pltpu.CompilerParams(collective_id=0, has_side_effects=True),
        )(query, k_cache, v_cache, k_new, v_new, lens)

        vr = lax.all_to_all(vt, "tp", 0, 0, tiled=True)

        whole = jax.ShapeDtypeStruct((batch, seq_local, n, head_dim), dtype)
        new_wide = pltpu.VMEM((batch * n, head_dim), jnp.float32)
        steps = 8
        in_block = lambda count: pl.BlockSpec((n, count // steps, seq_local, head_dim), lambda i: (0, i, 0, 0))
        out_block = lambda count: pl.BlockSpec((count // steps, seq_local, n, head_dim), lambda i: (i, 0, 0, 0))
        attn, k_out, v_out = pl.pallas_call(
            functools.partial(relayout_kernel, n),
            name="relayout",
            grid=(steps,),
            out_shape=[head_shape, whole, whole],
            in_specs=[smem_spec, vmem_spec, in_block(batch), in_block(batch - TAIL), vmem_spec, vmem_spec],
            out_specs=[vmem_spec, out_block(batch), out_block(batch - TAIL)],
            scratch_shapes=[new_wide, new_wide],
            cost_estimate=pl.CostEstimate(flops=10**10, bytes_accessed=4 * kx.size + 4 * vx.size, transcendentals=0),
        )(lens, attn, kx, vx, knx, vnx)

        block = 2
        first = batch - TAIL
        v_out = pl.pallas_call(
            functools.partial(tail_kernel, n, first),
            name="relayout_tail",
            grid=(TAIL // block,),
            out_shape=whole,
            in_specs=[smem_spec, vmem_spec, vmem_spec, any_spec],
            out_specs=pl.BlockSpec((block, seq_local, n, head_dim), lambda i: (first // block + i, 0, 0, 0)),
            scratch_shapes=[new_wide],
            input_output_aliases={3: 0},
            compiler_params=pltpu.CompilerParams(vmem_limit_bytes=8 * 2**20),
        )(lens, vr, vnx, v_out)
        return attn, k_out, v_out

    head_spec = P("dp", "tp")
    entry_spec = P("dp", None, "tp")
    return jax.shard_map(local_step, mesh=mesh, in_specs=(head_spec, entry_spec, entry_spec, head_spec, head_spec, P("dp")), out_specs=(head_spec, P("dp", "tp"), P("dp", "tp")), check_vma=False)
```

```python
import functools

import jax
import jax.numpy as jnp
from jax import lax
from jax.experimental import pallas as pl
from jax.experimental.pallas import tpu as pltpu
from jax.sharding import PartitionSpec as P


MASK_VALUE = -1e30
CHUNKS = ((0, 0, 16, 8), (0, 16, 48, 8), (1, 0, 40, 8), (1, 40, 16, 8), (1, 56, 6, 2), (1, 62, 2, 1))


def offsets(n):
    chips = n // 2
    far = chips // 2
    near = [h for h in range(1, chips) if h != far]
    return [(far, False), (far, True)] + [(h, False) for h in near] + [(h, True) for h in near] + [(0, True)]


def pairs(n, hops, other):
    return [(2 * c + k, 2 * ((c + hops) % (n // 2)) + ((1 - k) if other else k)) for c in range(n // 2) for k in range(2)]


def at(n, me, hops, other):
    chip = me // 2
    core = me - 2 * chip
    return 2 * lax.rem(chip + hops, n // 2) + (1 - core if other else core)


def pack_kernel(n, peers, first, pieces, lens_ref, src_ref, new_ref, *refs):
    outs, (buf, new_buf, new32, in_sem, out_sem, new_sem) = refs[:len(peers)], refs[len(peers):]
    count, seq_local = outs[0].shape[0], outs[0].shape[1]
    size = count // pieces
    me = lax.axis_index("tp")
    new_copy = pltpu.make_async_copy(new_ref, new_buf, new_sem)
    new_copy.start()
    slots = buf.shape[0]
    work = [(o, c) for o in range(len(peers)) for c in range(pieces)]

    def base(o):
        return pl.multiple_of(at(n, me, *peers[o]) * seq_local, seq_local)

    def load(w):
        o, c = work[w]
        return pltpu.make_async_copy(src_ref.at[pl.ds(first + c * size, size), pl.ds(base(o), seq_local)],
                                     buf.at[w % slots, pl.ds(0, size)], in_sem.at[w % slots])

    def store(w):
        o, c = work[w]
        return pltpu.make_async_copy(buf.at[w % slots, pl.ds(0, size)], outs[o].at[pl.ds(c * size, size)], out_sem.at[w % slots])

    ahead = slots // 2
    for w in range(min(ahead, len(work))):
        load(w).start()
    new_copy.wait()
    new32[...] = new_buf[...].astype(jnp.float32)
    positions = lax.broadcasted_iota(jnp.int32, (seq_local, 1), 0)
    for w, (o, c) in enumerate(work):
        if w + ahead < len(work):
            if w + ahead >= slots:
                store(w + ahead - slots).wait()
            load(w + ahead).start()
        load(w).wait()
        start = base(o)

        def patch(i, carry):
            b = first + c * size + i
            row = lens_ref[b] - start

            @pl.when((row >= 0) & (row < seq_local))
            def _():
                old = buf[w % slots, i]
                buf[w % slots, i] = jnp.where(positions == row, new32[pl.ds(b, 1), :], old.astype(jnp.float32)).astype(old.dtype)

            return carry

        lax.fori_loop(0, size, patch, 0, unroll=min(size, 8))
        store(w).start()
    for w in range(max(0, len(work) - slots), len(work)):
        store(w).wait()


def pack_first_kernel(n, peer, lens_ref, src_ref, new_ref, out_ref, lens_buf, new_buf, new32, sem):
    count, seq_local = out_ref.shape[0], out_ref.shape[1]
    start = pl.multiple_of(at(n, lax.axis_index("tp"), *peer) * seq_local, seq_local)
    data = pltpu.make_async_copy(src_ref.at[pl.ds(0, count), pl.ds(start, seq_local)], out_ref, sem.at[0])
    lengths = pltpu.make_async_copy(lens_ref, lens_buf, sem.at[1])
    new = pltpu.make_async_copy(new_ref, new_buf, sem.at[2])
    for copy in (lengths, new, data):
        copy.start()
    new.wait()
    new32[...] = new_buf[...].astype(jnp.float32)
    lengths.wait()
    data.wait()
    positions = lax.broadcasted_iota(jnp.int32, (seq_local, 1), 0)
    for b in range(count):
        row = lens_buf[b] - start

        @pl.when((row >= 0) & (row < seq_local))
        def _():
            old = out_ref[b]
            out_ref[b] = jnp.where(positions == row, new32[b:b + 1, :], old.astype(jnp.float32)).astype(old.dtype)


def pack_first(n, lens, src, new, peer, count):
    _, seq_len, head_dim = src.shape
    any_spec = pl.BlockSpec(memory_space=pl.ANY)
    return pl.pallas_call(
        functools.partial(pack_first_kernel, n, peer),
        name="pack_first",
        out_shape=pltpu.VMEM((count, seq_len // n, head_dim), src.dtype),
        in_specs=[any_spec] * 3,
        out_specs=pl.BlockSpec(memory_space=pltpu.VMEM),
        scratch_shapes=[pltpu.SMEM(lens.shape, lens.dtype), pltpu.VMEM(new.shape, new.dtype),
                        pltpu.VMEM(new.shape, jnp.float32), pltpu.SemaphoreType.DMA((3,))],
        cost_estimate=pl.CostEstimate(flops=count * 4_000_000, bytes_accessed=4 * count * seq_len // n * head_dim, transcendentals=0),
    )(lens, src, new)


def pack(n, lens, src, new, peers, first, count, pieces, slots):
    _, seq_len, head_dim = src.shape
    seq_local = seq_len // n
    any_spec = pl.BlockSpec(memory_space=pl.ANY)
    size = count // pieces
    return pl.pallas_call(
        functools.partial(pack_kernel, n, peers, first, pieces),
        out_shape=[jax.ShapeDtypeStruct((count, seq_local, head_dim), src.dtype)] * len(peers),
        in_specs=[pl.BlockSpec(memory_space=pltpu.SMEM), any_spec, any_spec],
        out_specs=[any_spec] * len(peers),
        scratch_shapes=[pltpu.VMEM((slots, size, seq_local, head_dim), src.dtype), pltpu.VMEM(new.shape, new.dtype),
                        pltpu.VMEM(new.shape, jnp.float32), pltpu.SemaphoreType.DMA((slots,)), pltpu.SemaphoreType.DMA((slots,)), pltpu.SemaphoreType.DMA],
        cost_estimate=pl.CostEstimate(flops=len(peers) * count * 4_000_000, bytes_accessed=4 * len(peers) * count * seq_local * head_dim, transcendentals=0),
    )(lens, src, new)


def attend_kernel(lens_ref, q_ref, k_ref, v_ref, kn_ref, vn_ref, out_ref, kn32, vn32):
    step = pl.program_id(0)
    block, seq_len, head_dim = k_ref.shape

    @pl.when(step == 0)
    def _():
        kn32[...] = kn_ref[...].astype(jnp.float32)
        vn32[...] = vn_ref[...].astype(jnp.float32)

    scale = head_dim ** -0.5
    positions = lax.broadcasted_iota(jnp.int32, (1, seq_len), 1)
    for i in range(block):
        b = step * block + i
        length = lens_ref[b]
        query = q_ref[i]
        new_k, new_v = kn32[pl.ds(b, 1), :], vn32[pl.ds(b, 1), :]
        scores = lax.dot_general(query, k_ref[i], (((1,), (1,)), ((), ())), preferred_element_type=jnp.float32)
        new_score = jnp.sum(query.astype(jnp.float32) * new_k, axis=-1, keepdims=True)
        is_new = positions == length
        scores = jnp.where(is_new, new_score, scores) * scale
        scores = jnp.where(positions <= length, scores, MASK_VALUE)
        weights = jnp.exp(scores - jnp.max(scores, axis=-1, keepdims=True))
        weights = weights / jnp.sum(weights, axis=-1, keepdims=True)
        probs = weights.astype(jnp.bfloat16)
        old = jnp.where(is_new, 0.0, weights).astype(jnp.bfloat16)
        summed = jnp.dot(old, v_ref[i], preferred_element_type=jnp.float32)
        new_prob = jnp.sum(jnp.where(is_new, probs.astype(jnp.float32), 0.0), axis=-1, keepdims=True)
        out_ref[i] = (summed + new_prob * new_v).astype(jnp.bfloat16)


def relayout_kernel(n, sources, *refs):
    xs, (o_ref, held) = refs[:n], refs[-2:]
    me = lax.axis_index("tp")
    block = o_ref.shape[0]
    for i in range(block):
        for x_ref, source in zip(xs, sources):
            row = i if x_ref.shape[0] == block else pl.program_id(0) * block + i
            held[i % 2, at(n, me, *source)] = x_ref[row]
        o_ref[i] = jnp.swapaxes(held[i % 2], 0, 1)


def relayout(n, sources, xs, whole, first, batch, block, resident=False):
    count, seq_local, head_dim = xs[0].shape
    return pl.pallas_call(
        functools.partial(relayout_kernel, n, sources),
        grid=(count // block,),
        out_shape=jax.ShapeDtypeStruct((batch, seq_local, n, head_dim), xs[0].dtype),
        in_specs=[pl.BlockSpec(memory_space=pltpu.VMEM) if resident else pl.BlockSpec((block, seq_local, head_dim), lambda i: (i, 0, 0))] * n
        + ([] if whole is None else [pl.BlockSpec(memory_space=pl.ANY)]),
        out_specs=pl.BlockSpec((block, seq_local, n, head_dim), lambda i: (first // block + i, 0, 0, 0)),
        scratch_shapes=[pltpu.VMEM((2, n, seq_local, head_dim), xs[0].dtype)],
        input_output_aliases={} if whole is None else {n: 0},
        compiler_params=pltpu.CompilerParams(vmem_limit_bytes=8 * 2**20) if resident else None,
        cost_estimate=pl.CostEstimate(flops=count * 40_000_000, bytes_accessed=4 * n * xs[0].size, transcendentals=0),
    )(*xs, *([] if whole is None else [whole]))


def solution(mesh):
    n = mesh.shape["tp"]
    peers = offsets(n)
    sources = [((n // 2 - h) % (n // 2), o) for h, o in peers] + [(0, False)]

    def local_step(query, k_cache, v_cache, k_new, v_new, lens):
        batch, seq_len, _, head_dim = k_cache.shape
        k_cache = k_cache.reshape(batch, seq_len, head_dim)
        v_cache = v_cache.reshape(batch, seq_len, head_dim)
        k_new = k_new.reshape(batch, head_dim)
        v_new = v_new.reshape(batch, head_dim)

        caches, news = (k_cache, v_cache), (k_new, v_new)
        own = [(0, False)]
        got = []
        for c, (a, first, count, _) in enumerate(CHUNKS):
            slabs = []
            if c == 0:
                slabs.append(pack_first(n, lens, caches[a], news[a], peers[0], count))
            pieces = 2 if count > 32 else 1
            slabs += pack(n, lens, caches[a], news[a], peers[len(slabs):] + own, first, count, pieces, 4)
            for i, peer in enumerate(peers):
                slabs[i] = lax.ppermute(slabs[i], "tp", pairs(n, *peer))
            got.append(slabs)

        block = 4
        cache_block = pl.BlockSpec((block, seq_len, head_dim), lambda i: (i, 0, 0))
        head_block = pl.BlockSpec((block,) + query.shape[1:], lambda i: (i, 0, 0))
        vmem_spec = pl.BlockSpec(memory_space=pltpu.VMEM)
        attend = pl.pallas_call(
            attend_kernel,
            name="attend",
            grid=(batch // block,),
            out_shape=jax.ShapeDtypeStruct(query.shape, query.dtype),
            in_specs=[pl.BlockSpec(memory_space=pltpu.SMEM), head_block, cache_block, cache_block, vmem_spec, vmem_spec],
            out_specs=head_block,
            scratch_shapes=[pltpu.VMEM((batch, head_dim), jnp.float32)] * 2,
            cost_estimate=pl.CostEstimate(flops=10**11, bytes_accessed=4 * k_cache.size, transcendentals=0),
        )
        attn = attend(lens, query, k_cache, v_cache, k_new, v_new)

        moved = [None, None]
        for c, (a, first, count, size) in enumerate(CHUNKS):
            moved[a] = relayout(n, sources, got[c], moved[a], first, batch, size, resident=c + 1 == len(CHUNKS))
        return attn, *moved


    head_spec = P("dp", "tp")
    entry_spec = P("dp", None, "tp")
    return jax.shard_map(local_step, mesh=mesh, in_specs=(head_spec, entry_spec, entry_spec, head_spec, head_spec, P("dp")), out_specs=(head_spec, P("dp", "tp"), P("dp", "tp")), check_vma=False)
```

```python
import functools

import jax
import jax.numpy as jnp
from jax import lax
from jax.experimental import pallas as pl
from jax.experimental.pallas import tpu as pltpu
from jax.sharding import PartitionSpec as P


MASK_VALUE = -1e30
CHUNKS = ((0, 0, 20, 4), (0, 20, 44, 4), (1, 12, 50, 2), (1, 0, 12, 6), (1, 62, 2, 2))
ROOM = pltpu.CompilerParams(vmem_limit_bytes=65_900_000)


def offsets(n):
    chips = n // 2
    far = chips // 2
    near = [h for h in range(1, chips) if h != far]
    return [(far, False), (far, True)] + [(h, False) for h in near] + [(h, True) for h in near] + [(0, True)]


def pairs(n, hops, other):
    return [(2 * c + k, 2 * ((c + hops) % (n // 2)) + ((1 - k) if other else k)) for c in range(n // 2) for k in range(2)]


def at(n, me, hops, other):
    chip = me // 2
    core = me - 2 * chip
    return 2 * lax.rem(chip + hops, n // 2) + (1 - core if other else core)


def pack_kernel(n, peers, first, pieces, lens_ref, src_ref, new_ref, *refs):
    outs, (buf, new_buf, new32, in_sem, out_sem, new_sem) = refs[:len(peers)], refs[len(peers):]
    count, seq_local = outs[0].shape[0], outs[0].shape[1]
    size = count // pieces
    me = lax.axis_index("tp")
    new_copy = pltpu.make_async_copy(new_ref, new_buf, new_sem)
    new_copy.start()
    slots = buf.shape[0]
    work = [(o, c) for o in range(len(peers)) for c in range(pieces)]

    def base(o):
        return pl.multiple_of(at(n, me, *peers[o]) * seq_local, seq_local)

    def load(w):
        o, c = work[w]
        return pltpu.make_async_copy(src_ref.at[pl.ds(first + c * size, size), pl.ds(base(o), seq_local)],
                                     buf.at[w % slots, pl.ds(0, size)], in_sem.at[w % slots])

    def store(w):
        o, c = work[w]
        return pltpu.make_async_copy(buf.at[w % slots, pl.ds(0, size)], outs[o].at[pl.ds(c * size, size)], out_sem.at[w % slots])

    ahead = slots // 2
    for w in range(min(ahead, len(work))):
        load(w).start()
    new_copy.wait()
    new32[...] = new_buf[...].astype(jnp.float32)
    positions = lax.broadcasted_iota(jnp.int32, (seq_local, 1), 0)
    for w, (o, c) in enumerate(work):
        if w + ahead < len(work):
            if w + ahead >= slots:
                store(w + ahead - slots).wait()
            load(w + ahead).start()
        load(w).wait()
        start = base(o)

        def patch(i, carry):
            b = first + c * size + i
            row = lens_ref[b] - start

            @pl.when((row >= 0) & (row < seq_local))
            def _():
                old = buf[w % slots, i]
                buf[w % slots, i] = jnp.where(positions == row, new32[pl.ds(b, 1), :], old.astype(jnp.float32)).astype(old.dtype)

            return carry

        lax.fori_loop(0, size, patch, 0, unroll=min(size, 8))
        store(w).start()
    for w in range(max(0, len(work) - slots), len(work)):
        store(w).wait()


def pack_first_kernel(n, peer, lens_ref, src_ref, new_ref, out_ref, lens_buf, new_buf, new32, sem):
    count, seq_local = out_ref.shape[0], out_ref.shape[1]
    start = pl.multiple_of(at(n, lax.axis_index("tp"), *peer) * seq_local, seq_local)
    data = pltpu.make_async_copy(src_ref.at[pl.ds(0, count), pl.ds(start, seq_local)], out_ref, sem.at[0])
    lengths = pltpu.make_async_copy(lens_ref, lens_buf, sem.at[1])
    new = pltpu.make_async_copy(new_ref, new_buf, sem.at[2])
    for copy in (lengths, new, data):
        copy.start()
    new.wait()
    new32[...] = new_buf[...].astype(jnp.float32)
    lengths.wait()
    data.wait()
    positions = lax.broadcasted_iota(jnp.int32, (seq_local, 1), 0)
    for b in range(count):
        row = lens_buf[b] - start

        @pl.when((row >= 0) & (row < seq_local))
        def _():
            old = out_ref[b]
            out_ref[b] = jnp.where(positions == row, new32[b:b + 1, :], old.astype(jnp.float32)).astype(old.dtype)


def pack_first(n, lens, src, new, peer, count):
    _, seq_len, head_dim = src.shape
    any_spec = pl.BlockSpec(memory_space=pl.ANY)
    return pl.pallas_call(
        functools.partial(pack_first_kernel, n, peer),
        name="pack_first",
        out_shape=pltpu.VMEM((count, seq_len // n, head_dim), src.dtype),
        in_specs=[any_spec] * 3,
        out_specs=pl.BlockSpec(memory_space=pltpu.VMEM),
        scratch_shapes=[pltpu.SMEM(lens.shape, lens.dtype), pltpu.VMEM(new.shape, new.dtype),
                        pltpu.VMEM(new.shape, jnp.float32), pltpu.SemaphoreType.DMA((3,))],
        compiler_params=ROOM,
        cost_estimate=pl.CostEstimate(flops=count * 4_000_000, bytes_accessed=4 * count * seq_len // n * head_dim, transcendentals=0),
    )(lens, src, new)


def pack(n, lens, src, new, peers, first, count, pieces, slots):
    _, seq_len, head_dim = src.shape
    seq_local = seq_len // n
    any_spec = pl.BlockSpec(memory_space=pl.ANY)
    size = count // pieces
    return pl.pallas_call(
        functools.partial(pack_kernel, n, peers, first, pieces),
        out_shape=[jax.ShapeDtypeStruct((count, seq_local, head_dim), src.dtype)] * len(peers),
        in_specs=[pl.BlockSpec(memory_space=pltpu.SMEM), any_spec, any_spec],
        out_specs=[any_spec] * len(peers),
        scratch_shapes=[pltpu.VMEM((slots, size, seq_local, head_dim), src.dtype), pltpu.VMEM(new.shape, new.dtype),
                        pltpu.VMEM(new.shape, jnp.float32), pltpu.SemaphoreType.DMA((slots,)), pltpu.SemaphoreType.DMA((slots,)), pltpu.SemaphoreType.DMA],
        compiler_params=ROOM,
        cost_estimate=pl.CostEstimate(flops=len(peers) * count * 4_000_000, bytes_accessed=4 * len(peers) * count * seq_local * head_dim, transcendentals=0),
    )(lens, src, new)


def attend_kernel(lens_ref, q_ref, k_ref, v_ref, kn_ref, vn_ref, out_ref, kn32, vn32):
    step = pl.program_id(0)
    block, seq_len, head_dim = k_ref.shape

    @pl.when(step == 0)
    def _():
        kn32[...] = kn_ref[...].astype(jnp.float32)
        vn32[...] = vn_ref[...].astype(jnp.float32)

    scale = head_dim ** -0.5
    positions = lax.broadcasted_iota(jnp.int32, (1, seq_len), 1)
    for i in range(block):
        b = step * block + i
        length = lens_ref[b]
        query = q_ref[i]
        new_k, new_v = kn32[pl.ds(b, 1), :], vn32[pl.ds(b, 1), :]
        scores = lax.dot_general(query, k_ref[i], (((1,), (1,)), ((), ())), preferred_element_type=jnp.float32)
        new_score = jnp.sum(query.astype(jnp.float32) * new_k, axis=-1, keepdims=True)
        is_new = positions == length
        scores = jnp.where(is_new, new_score, scores) * scale
        scores = jnp.where(positions <= length, scores, MASK_VALUE)
        weights = jnp.exp(scores - jnp.max(scores, axis=-1, keepdims=True))
        weights = weights / jnp.sum(weights, axis=-1, keepdims=True)
        probs = weights.astype(jnp.bfloat16)
        old = jnp.where(is_new, 0.0, weights).astype(jnp.bfloat16)
        summed = jnp.dot(old, v_ref[i], preferred_element_type=jnp.float32)
        new_prob = jnp.sum(jnp.where(is_new, probs.astype(jnp.float32), 0.0), axis=-1, keepdims=True)
        out_ref[i] = (summed + new_prob * new_v).astype(jnp.bfloat16)


def relayout_kernel(n, sources, *refs):
    xs, (o_ref, held) = refs[:n], refs[-2:]
    me = lax.axis_index("tp")
    for i in range(o_ref.shape[0]):
        for x_ref, source in zip(xs, sources):
            held[i % 2, at(n, me, *source)] = x_ref[i]
        o_ref[i] = jnp.swapaxes(held[i % 2], 0, 1)


def relayout(n, sources, xs, whole, first, batch, block):
    count, seq_local, head_dim = xs[0].shape
    return pl.pallas_call(
        functools.partial(relayout_kernel, n, sources),
        grid=(count // block,),
        out_shape=jax.ShapeDtypeStruct((batch, seq_local, n, head_dim), xs[0].dtype),
        in_specs=[pl.BlockSpec((block, seq_local, head_dim), lambda i: (i, 0, 0))] * n
        + ([] if whole is None else [pl.BlockSpec(memory_space=pl.ANY)]),
        out_specs=pl.BlockSpec((block, seq_local, n, head_dim), lambda i: (first // block + i, 0, 0, 0)),
        scratch_shapes=[pltpu.VMEM((2, n, seq_local, head_dim), xs[0].dtype)],
        input_output_aliases={} if whole is None else {n: 0},
        compiler_params=ROOM,
        cost_estimate=pl.CostEstimate(flops=count * 40_000_000, bytes_accessed=4 * n * xs[0].size, transcendentals=0),
    )(*xs, *([] if whole is None else [whole]))


def last_relayout_kernel(n, sources, first, *refs):
    xs, (o_ref, held, ready, sem) = refs[:n], refs[-4:]
    me = lax.axis_index("tp")
    copies = []
    for i in range(ready.shape[0]):
        for x_ref, source in zip(xs, sources):
            held[i, at(n, me, *source)] = x_ref[i]
        ready[i] = jnp.swapaxes(held[i], 0, 1)
        copies.append(pltpu.make_async_copy(ready.at[i], o_ref.at[first + i], sem.at[i]))
        copies[-1].start()
    for copy in copies:
        copy.wait()


def last_relayout(n, sources, xs, whole, first):
    count, seq_local, head_dim = xs[0].shape
    return pl.pallas_call(
        functools.partial(last_relayout_kernel, n, sources, first),
        out_shape=jax.ShapeDtypeStruct(whole.shape, whole.dtype),
        in_specs=[pl.BlockSpec(memory_space=pltpu.VMEM)] * n + [pl.BlockSpec(memory_space=pl.ANY)],
        out_specs=pl.BlockSpec(memory_space=pl.ANY),
        scratch_shapes=[pltpu.VMEM((count, n, seq_local, head_dim), whole.dtype), pltpu.VMEM((count, seq_local, n, head_dim), whole.dtype),
                        pltpu.SemaphoreType.DMA((count,))],
        input_output_aliases={n: 0},
        compiler_params=pltpu.CompilerParams(vmem_limit_bytes=8 * 2**20),
    )(*xs, whole)


def solution(mesh):
    n = mesh.shape["tp"]
    peers = offsets(n)
    sources = [((n // 2 - h) % (n // 2), o) for h, o in peers] + [(0, False)]

    def local_step(query, k_cache, v_cache, k_new, v_new, lens):
        batch, seq_len, _, head_dim = k_cache.shape
        k_cache = k_cache.reshape(batch, seq_len, head_dim)
        v_cache = v_cache.reshape(batch, seq_len, head_dim)
        k_new = k_new.reshape(batch, head_dim)
        v_new = v_new.reshape(batch, head_dim)

        caches, news = (k_cache, v_cache), (k_new, v_new)
        own = [(0, False)]
        got = []
        for c, (a, first, count, _) in enumerate(CHUNKS):
            slabs = []
            if c == 0:
                slabs.append(pack_first(n, lens, caches[a], news[a], peers[0], count))
            pieces = 2 if count > 32 else 1
            slabs += pack(n, lens, caches[a], news[a], peers[len(slabs):] + own, first, count, pieces, 4)
            for i, peer in enumerate(peers):
                slabs[i] = lax.ppermute(slabs[i], "tp", pairs(n, *peer))
            got.append(slabs)

        block = 4
        cache_block = pl.BlockSpec((block, seq_len, head_dim), lambda i: (i, 0, 0))
        head_block = pl.BlockSpec((block,) + query.shape[1:], lambda i: (i, 0, 0))
        vmem_spec = pl.BlockSpec(memory_space=pltpu.VMEM)
        attend = pl.pallas_call(
            attend_kernel,
            name="attend",
            grid=(batch // block,),
            out_shape=jax.ShapeDtypeStruct(query.shape, query.dtype),
            in_specs=[pl.BlockSpec(memory_space=pltpu.SMEM), head_block, cache_block, cache_block, vmem_spec, vmem_spec],
            out_specs=head_block,
            scratch_shapes=[pltpu.VMEM((batch, head_dim), jnp.float32)] * 2,
            compiler_params=ROOM,
            cost_estimate=pl.CostEstimate(flops=10**11, bytes_accessed=4 * k_cache.size, transcendentals=0),
        )
        attn = attend(lens, query, k_cache, v_cache, k_new, v_new)

        moved = [None, None]
        for c, (a, first, count, size) in enumerate(CHUNKS):
            if c + 1 < len(CHUNKS):
                moved[a] = relayout(n, sources, got[c], moved[a], first, batch, size)
            else:
                moved[a] = last_relayout(n, sources, got[c], moved[a], first)
        return attn, *moved


    head_spec = P("dp", "tp")
    entry_spec = P("dp", None, "tp")
    return jax.shard_map(local_step, mesh=mesh, in_specs=(head_spec, entry_spec, entry_spec, head_spec, head_spec, P("dp")), out_specs=(head_spec, P("dp", "tp"), P("dp", "tp")), check_vma=False)
```

```python
import functools

import jax
import jax.numpy as jnp
from jax import lax
from jax.experimental import pallas as pl
from jax.experimental.pallas import tpu as pltpu
from jax.sharding import PartitionSpec as P


MASK_VALUE = -1e30
CHUNKS = ((0, 0, 16, 16), (0, 16, 48, 16), (1, 12, 48, 12), (1, 0, 12, 6), (1, 60, 4, 4))
ROOM = pltpu.CompilerParams(vmem_limit_bytes=65_520_000)


def offsets(n):
    chips = n // 2
    far = chips // 2
    near = [h for h in range(1, chips) if h != far]
    return [(far, False), (far, True)] + [(h, False) for h in near] + [(h, True) for h in near] + [(0, True)]


def pairs(n, hops, other):
    return [(2 * c + k, 2 * ((c + hops) % (n // 2)) + ((1 - k) if other else k)) for c in range(n // 2) for k in range(2)]


def at(n, me, hops, other):
    chip = me // 2
    core = me - 2 * chip
    return 2 * lax.rem(chip + hops, n // 2) + (1 - core if other else core)


def pack_kernel(n, peers, first, pieces, lens_ref, src_ref, new_ref, *refs):
    outs, (buf, new_buf, new32, in_sem, out_sem, new_sem) = refs[:len(peers)], refs[len(peers):]
    count, seq_local = outs[0].shape[0], outs[0].shape[1]
    size = count // pieces
    me = lax.axis_index("tp")
    new_copy = pltpu.make_async_copy(new_ref, new_buf, new_sem)
    new_copy.start()
    slots = buf.shape[0]
    work = [(o, c) for o in range(len(peers)) for c in range(pieces)]

    def base(o):
        return pl.multiple_of(at(n, me, *peers[o]) * seq_local, seq_local)

    def load(w):
        o, c = work[w]
        return pltpu.make_async_copy(src_ref.at[pl.ds(first + c * size, size), pl.ds(base(o), seq_local)],
                                     buf.at[w % slots, pl.ds(0, size)], in_sem.at[w % slots])

    def store(w):
        o, c = work[w]
        return pltpu.make_async_copy(buf.at[w % slots, pl.ds(0, size)], outs[o].at[pl.ds(c * size, size)], out_sem.at[w % slots])

    ahead = slots // 2
    for w in range(min(ahead, len(work))):
        load(w).start()
    new_copy.wait()
    new32[...] = new_buf[...].astype(jnp.float32)
    positions = lax.broadcasted_iota(jnp.int32, (seq_local, 1), 0)
    for w, (o, c) in enumerate(work):
        if w + ahead < len(work):
            if w + ahead >= slots:
                store(w + ahead - slots).wait()
            load(w + ahead).start()
        load(w).wait()
        start = base(o)

        def patch(i, carry):
            b = first + c * size + i
            row = lens_ref[b] - start

            @pl.when((row >= 0) & (row < seq_local))
            def _():
                old = buf[w % slots, i]
                buf[w % slots, i] = jnp.where(positions == row, new32[pl.ds(b, 1), :], old.astype(jnp.float32)).astype(old.dtype)

            return carry

        lax.fori_loop(0, size, patch, 0, unroll=min(size, 8))
        store(w).start()
    for w in range(max(0, len(work) - slots), len(work)):
        store(w).wait()


def pack_first_kernel(n, peer, lens_ref, src_ref, new_ref, out_ref, lens_buf, new_buf, new32, sem):
    count, seq_local = out_ref.shape[0], out_ref.shape[1]
    start = pl.multiple_of(at(n, lax.axis_index("tp"), *peer) * seq_local, seq_local)
    data = pltpu.make_async_copy(src_ref.at[pl.ds(0, count), pl.ds(start, seq_local)], out_ref, sem.at[0])
    lengths = pltpu.make_async_copy(lens_ref, lens_buf, sem.at[1])
    new = pltpu.make_async_copy(new_ref, new_buf, sem.at[2])
    for copy in (lengths, new, data):
        copy.start()
    new.wait()
    new32[...] = new_buf[...].astype(jnp.float32)
    lengths.wait()
    data.wait()
    positions = lax.broadcasted_iota(jnp.int32, (seq_local, 1), 0)
    for b in range(count):
        row = lens_buf[b] - start

        @pl.when((row >= 0) & (row < seq_local))
        def _():
            old = out_ref[b]
            out_ref[b] = jnp.where(positions == row, new32[b:b + 1, :], old.astype(jnp.float32)).astype(old.dtype)


def pack_first(n, lens, src, new, peer, count):
    _, seq_len, head_dim = src.shape
    any_spec = pl.BlockSpec(memory_space=pl.ANY)
    return pl.pallas_call(
        functools.partial(pack_first_kernel, n, peer),
        name="pack_first",
        out_shape=pltpu.VMEM((count, seq_len // n, head_dim), src.dtype),
        in_specs=[any_spec] * 3,
        out_specs=pl.BlockSpec(memory_space=pltpu.VMEM),
        scratch_shapes=[pltpu.SMEM(lens.shape, lens.dtype), pltpu.VMEM(new.shape, new.dtype),
                        pltpu.VMEM(new.shape, jnp.float32), pltpu.SemaphoreType.DMA((3,))],
        compiler_params=ROOM,
        cost_estimate=pl.CostEstimate(flops=count * 4_000_000, bytes_accessed=4 * count * seq_len // n * head_dim, transcendentals=0),
    )(lens, src, new)


def pack(n, lens, src, new, peers, first, count, pieces, slots):
    _, seq_len, head_dim = src.shape
    seq_local = seq_len // n
    any_spec = pl.BlockSpec(memory_space=pl.ANY)
    size = count // pieces
    return pl.pallas_call(
        functools.partial(pack_kernel, n, peers, first, pieces),
        out_shape=[jax.ShapeDtypeStruct((count, seq_local, head_dim), src.dtype)] * len(peers),
        in_specs=[pl.BlockSpec(memory_space=pltpu.SMEM), any_spec, any_spec],
        out_specs=[any_spec] * len(peers),
        scratch_shapes=[pltpu.VMEM((slots, size, seq_local, head_dim), src.dtype), pltpu.VMEM(new.shape, new.dtype),
                        pltpu.VMEM(new.shape, jnp.float32), pltpu.SemaphoreType.DMA((slots,)), pltpu.SemaphoreType.DMA((slots,)), pltpu.SemaphoreType.DMA],
        compiler_params=ROOM,
        cost_estimate=pl.CostEstimate(flops=len(peers) * count * 4_000_000, bytes_accessed=4 * len(peers) * count * seq_local * head_dim, transcendentals=0),
    )(lens, src, new)


def attend_kernel(lens_ref, q_ref, k_ref, v_ref, kn_ref, vn_ref, out_ref, kn32, vn32):
    step = pl.program_id(0)
    block, seq_len, head_dim = k_ref.shape

    @pl.when(step == 0)
    def _():
        kn32[...] = kn_ref[...].astype(jnp.float32)
        vn32[...] = vn_ref[...].astype(jnp.float32)

    scale = head_dim ** -0.5
    positions = lax.broadcasted_iota(jnp.int32, (1, seq_len), 1)
    for i in range(block):
        b = step * block + i
        length = lens_ref[b]
        query = q_ref[i]
        new_k, new_v = kn32[pl.ds(b, 1), :], vn32[pl.ds(b, 1), :]
        scores = lax.dot_general(query, k_ref[i], (((1,), (1,)), ((), ())), preferred_element_type=jnp.float32)
        new_score = jnp.sum(query.astype(jnp.float32) * new_k, axis=-1, keepdims=True)
        is_new = positions == length
        scores = jnp.where(is_new, new_score, scores) * scale
        scores = jnp.where(positions <= length, scores, MASK_VALUE)
        weights = jnp.exp(scores - jnp.max(scores, axis=-1, keepdims=True))
        weights = weights / jnp.sum(weights, axis=-1, keepdims=True)
        probs = weights.astype(jnp.bfloat16)
        old = jnp.where(is_new, 0.0, weights).astype(jnp.bfloat16)
        summed = jnp.dot(old, v_ref[i], preferred_element_type=jnp.float32)
        new_prob = jnp.sum(jnp.where(is_new, probs.astype(jnp.float32), 0.0), axis=-1, keepdims=True)
        out_ref[i] = (summed + new_prob * new_v).astype(jnp.bfloat16)


def relayout_kernel(n, sources, *refs):
    xs, (o_ref, held) = refs[:n], refs[-2:]
    me = lax.axis_index("tp")
    for i in range(o_ref.shape[0]):
        for x_ref, source in zip(xs, sources):
            held[i % 2, at(n, me, *source)] = x_ref[i]
        o_ref[i] = jnp.swapaxes(held[i % 2], 0, 1)


def relayout(n, sources, xs, whole, first, batch, block):
    count, seq_local, head_dim = xs[0].shape
    return pl.pallas_call(
        functools.partial(relayout_kernel, n, sources),
        grid=(count // block,),
        out_shape=jax.ShapeDtypeStruct((batch, seq_local, n, head_dim), xs[0].dtype),
        in_specs=[pl.BlockSpec((block, seq_local, head_dim), lambda i: (i, 0, 0))] * n
        + ([] if whole is None else [pl.BlockSpec(memory_space=pl.ANY)]),
        out_specs=pl.BlockSpec((block, seq_local, n, head_dim), lambda i: (first // block + i, 0, 0, 0)),
        scratch_shapes=[pltpu.VMEM((2, n, seq_local, head_dim), xs[0].dtype)],
        input_output_aliases={} if whole is None else {n: 0},
        compiler_params=ROOM,
        cost_estimate=pl.CostEstimate(flops=count * 40_000_000, bytes_accessed=4 * n * xs[0].size, transcendentals=0),
    )(*xs, *([] if whole is None else [whole]))


def last_relayout_kernel(n, sources, first, *refs):
    xs, (o_ref, held, ready, sem) = refs[:n], refs[-4:]
    me = lax.axis_index("tp")
    copies = []
    for i in range(ready.shape[0]):
        for x_ref, source in zip(xs, sources):
            held[i, at(n, me, *source)] = x_ref[i]
        ready[i] = jnp.swapaxes(held[i], 0, 1)
        copies.append(pltpu.make_async_copy(ready.at[i], o_ref.at[first + i], sem.at[i]))
        copies[-1].start()
    for copy in copies:
        copy.wait()


def last_relayout(n, sources, xs, whole, first):
    count, seq_local, head_dim = xs[0].shape
    return pl.pallas_call(
        functools.partial(last_relayout_kernel, n, sources, first),
        out_shape=jax.ShapeDtypeStruct(whole.shape, whole.dtype),
        in_specs=[pl.BlockSpec(memory_space=pltpu.VMEM)] * n + [pl.BlockSpec(memory_space=pl.ANY)],
        out_specs=pl.BlockSpec(memory_space=pl.ANY),
        scratch_shapes=[pltpu.VMEM((count, n, seq_local, head_dim), whole.dtype), pltpu.VMEM((count, seq_local, n, head_dim), whole.dtype),
                        pltpu.SemaphoreType.DMA((count,))],
        input_output_aliases={n: 0},
        compiler_params=pltpu.CompilerParams(vmem_limit_bytes=8 * 2**20),
    )(*xs, whole)


def solution(mesh):
    n = mesh.shape["tp"]
    peers = offsets(n)
    sources = [((n // 2 - h) % (n // 2), o) for h, o in peers] + [(0, False)]

    def local_step(query, k_cache, v_cache, k_new, v_new, lens):
        batch, seq_len, _, head_dim = k_cache.shape
        k_cache = k_cache.reshape(batch, seq_len, head_dim)
        v_cache = v_cache.reshape(batch, seq_len, head_dim)
        k_new = k_new.reshape(batch, head_dim)
        v_new = v_new.reshape(batch, head_dim)

        caches, news = (k_cache, v_cache), (k_new, v_new)
        own = [(0, False)]
        got = []
        for c, (a, first, count, _) in enumerate(CHUNKS):
            slabs = []
            if c == 0:
                slabs.append(pack_first(n, lens, caches[a], news[a], peers[0], count))
            slabs += pack(n, lens, caches[a], news[a], peers[len(slabs):] + own, first, count, 1, 4)
            for i, peer in enumerate(peers):
                slabs[i] = lax.ppermute(slabs[i], "tp", pairs(n, *peer))
            got.append(slabs)

        block = 8
        cache_block = pl.BlockSpec((block, seq_len, head_dim), lambda i: (i, 0, 0))
        head_block = pl.BlockSpec((block,) + query.shape[1:], lambda i: (i, 0, 0))
        vmem_spec = pl.BlockSpec(memory_space=pltpu.VMEM)
        attend = pl.pallas_call(
            attend_kernel,
            name="attend",
            grid=(batch // block,),
            out_shape=jax.ShapeDtypeStruct(query.shape, query.dtype),
            in_specs=[pl.BlockSpec(memory_space=pltpu.SMEM), head_block, cache_block, cache_block, vmem_spec, vmem_spec],
            out_specs=head_block,
            scratch_shapes=[pltpu.VMEM((batch, head_dim), jnp.float32)] * 2,
            compiler_params=ROOM,
            cost_estimate=pl.CostEstimate(flops=10**11, bytes_accessed=4 * k_cache.size, transcendentals=0),
        )
        attn = attend(lens, query, k_cache, v_cache, k_new, v_new)

        moved = [None, None]
        for c, (a, first, count, size) in enumerate(CHUNKS):
            if c + 1 < len(CHUNKS):
                moved[a] = relayout(n, sources, got[c], moved[a], first, batch, size)
            else:
                moved[a] = last_relayout(n, sources, got[c], moved[a], first)
        return attn, *moved


    head_spec = P("dp", "tp")
    entry_spec = P("dp", None, "tp")
    return jax.shard_map(local_step, mesh=mesh, in_specs=(head_spec, entry_spec, entry_spec, head_spec, head_spec, P("dp")), out_specs=(head_spec, P("dp", "tp"), P("dp", "tp")), check_vma=False)
```

```python
import functools

import jax
import jax.numpy as jnp
from jax import lax
from jax.experimental import pallas as pl
from jax.experimental.pallas import tpu as pltpu
from jax.sharding import PartitionSpec as P


MASK_VALUE = -1e30
CHUNKS = ((0, 0, 16, 16), (0, 16, 48, 24), (1, 0, 50, 25), (1, 50, 12, 6), (1, 62, 2, 2))
ROOM = pltpu.CompilerParams(vmem_limit_bytes=66_000_000)


def offsets(n):
    chips = n // 2
    far = chips // 2
    near = [h for h in range(1, chips) if h != far]
    return [(far, False), (far, True)] + [(h, False) for h in near] + [(h, True) for h in near] + [(0, True)]


def pairs(n, hops, other):
    return [(2 * c + k, 2 * ((c + hops) % (n // 2)) + ((1 - k) if other else k)) for c in range(n // 2) for k in range(2)]


def at(n, me, hops, other):
    chip = me // 2
    core = me - 2 * chip
    return 2 * lax.rem(chip + hops, n // 2) + (1 - core if other else core)


def pack_kernel(n, peers, first, pieces, lens_ref, src_ref, new_ref, *refs):
    outs, (buf, new_buf, new32, in_sem, out_sem, new_sem) = refs[:len(peers)], refs[len(peers):]
    count, seq_local = outs[0].shape[0], outs[0].shape[1]
    size = count // pieces
    me = lax.axis_index("tp")
    new_copy = pltpu.make_async_copy(new_ref, new_buf, new_sem)
    new_copy.start()
    slots = buf.shape[0]
    work = [(o, c) for o in range(len(peers)) for c in range(pieces)]

    def base(o):
        return pl.multiple_of(at(n, me, *peers[o]) * seq_local, seq_local)

    def load(w):
        o, c = work[w]
        return pltpu.make_async_copy(src_ref.at[pl.ds(first + c * size, size), pl.ds(base(o), seq_local)],
                                     buf.at[w % slots, pl.ds(0, size)], in_sem.at[w % slots])

    def store(w):
        o, c = work[w]
        return pltpu.make_async_copy(buf.at[w % slots, pl.ds(0, size)], outs[o].at[pl.ds(c * size, size)], out_sem.at[w % slots])

    ahead = slots // 2
    for w in range(min(ahead, len(work))):
        load(w).start()
    new_copy.wait()
    new32[...] = new_buf[...].astype(jnp.float32)
    positions = lax.broadcasted_iota(jnp.int32, (seq_local, 1), 0)
    for w, (o, c) in enumerate(work):
        if w + ahead < len(work):
            if w + ahead >= slots:
                store(w + ahead - slots).wait()
            load(w + ahead).start()
        load(w).wait()
        start = base(o)

        def patch(i, carry):
            b = first + c * size + i
            row = lens_ref[b] - start

            @pl.when((row >= 0) & (row < seq_local))
            def _():
                old = buf[w % slots, i]
                buf[w % slots, i] = jnp.where(positions == row, new32[pl.ds(b, 1), :], old.astype(jnp.float32)).astype(old.dtype)

            return carry

        lax.fori_loop(0, size, patch, 0, unroll=min(size, 8))
        store(w).start()
    for w in range(max(0, len(work) - slots), len(work)):
        store(w).wait()


def pack_first_kernel(n, peer, lens_ref, src_ref, new_ref, out_ref, lens_buf, new_buf, new32, sem):
    count, seq_local = out_ref.shape[0], out_ref.shape[1]
    start = pl.multiple_of(at(n, lax.axis_index("tp"), *peer) * seq_local, seq_local)
    data = pltpu.make_async_copy(src_ref.at[pl.ds(0, count), pl.ds(start, seq_local)], out_ref, sem.at[0])
    lengths = pltpu.make_async_copy(lens_ref, lens_buf, sem.at[1])
    new = pltpu.make_async_copy(new_ref, new_buf, sem.at[2])
    for copy in (lengths, new, data):
        copy.start()
    new.wait()
    new32[...] = new_buf[...].astype(jnp.float32)
    lengths.wait()
    data.wait()
    positions = lax.broadcasted_iota(jnp.int32, (seq_local, 1), 0)
    for b in range(count):
        row = lens_buf[b] - start

        @pl.when((row >= 0) & (row < seq_local))
        def _():
            old = out_ref[b]
            out_ref[b] = jnp.where(positions == row, new32[b:b + 1, :], old.astype(jnp.float32)).astype(old.dtype)


def pack_first(n, lens, src, new, peer, count):
    _, seq_len, head_dim = src.shape
    any_spec = pl.BlockSpec(memory_space=pl.ANY)
    return pl.pallas_call(
        functools.partial(pack_first_kernel, n, peer),
        name="pack_first",
        out_shape=pltpu.VMEM((count, seq_len // n, head_dim), src.dtype),
        in_specs=[any_spec] * 3,
        out_specs=pl.BlockSpec(memory_space=pltpu.VMEM),
        scratch_shapes=[pltpu.SMEM(lens.shape, lens.dtype), pltpu.VMEM(new.shape, new.dtype),
                        pltpu.VMEM(new.shape, jnp.float32), pltpu.SemaphoreType.DMA((3,))],
        compiler_params=ROOM,
        cost_estimate=pl.CostEstimate(flops=count * 4_000_000, bytes_accessed=4 * count * seq_len // n * head_dim, transcendentals=0),
    )(lens, src, new)


def pack(n, lens, src, new, peers, first, count, pieces, slots):
    _, seq_len, head_dim = src.shape
    seq_local = seq_len // n
    any_spec = pl.BlockSpec(memory_space=pl.ANY)
    size = count // pieces
    return pl.pallas_call(
        functools.partial(pack_kernel, n, peers, first, pieces),
        out_shape=[jax.ShapeDtypeStruct((count, seq_local, head_dim), src.dtype)] * len(peers),
        in_specs=[pl.BlockSpec(memory_space=pltpu.SMEM), any_spec, any_spec],
        out_specs=[any_spec] * len(peers),
        scratch_shapes=[pltpu.VMEM((slots, size, seq_local, head_dim), src.dtype), pltpu.VMEM(new.shape, new.dtype),
                        pltpu.VMEM(new.shape, jnp.float32), pltpu.SemaphoreType.DMA((slots,)), pltpu.SemaphoreType.DMA((slots,)), pltpu.SemaphoreType.DMA],
        compiler_params=ROOM,
        cost_estimate=pl.CostEstimate(flops=len(peers) * count * 4_000_000, bytes_accessed=4 * len(peers) * count * seq_local * head_dim, transcendentals=0),
    )(lens, src, new)


def attend_kernel(lens_ref, q_ref, k_ref, v_ref, kn_ref, vn_ref, out_ref, kn32, vn32):
    step = pl.program_id(0)
    block, seq_len, head_dim = k_ref.shape

    @pl.when(step == 0)
    def _():
        kn32[...] = kn_ref[...].astype(jnp.float32)
        vn32[...] = vn_ref[...].astype(jnp.float32)

    scale = head_dim ** -0.5
    positions = lax.broadcasted_iota(jnp.int32, (1, seq_len), 1)
    for i in range(block):
        b = step * block + i
        length = lens_ref[b]
        query = q_ref[i]
        new_k, new_v = kn32[pl.ds(b, 1), :], vn32[pl.ds(b, 1), :]
        scores = lax.dot_general(query, k_ref[i], (((1,), (1,)), ((), ())), preferred_element_type=jnp.float32)
        new_score = jnp.sum(query.astype(jnp.float32) * new_k, axis=-1, keepdims=True)
        is_new = positions == length
        scores = jnp.where(is_new, new_score, scores) * scale
        scores = jnp.where(positions <= length, scores, MASK_VALUE)
        weights = jnp.exp(scores - jnp.max(scores, axis=-1, keepdims=True))
        weights = weights / jnp.sum(weights, axis=-1, keepdims=True)
        probs = weights.astype(jnp.bfloat16)
        old = jnp.where(is_new, 0.0, weights).astype(jnp.bfloat16)
        summed = jnp.dot(old, v_ref[i], preferred_element_type=jnp.float32)
        new_prob = jnp.sum(jnp.where(is_new, probs.astype(jnp.float32), 0.0), axis=-1, keepdims=True)
        out_ref[i] = (summed + new_prob * new_v).astype(jnp.bfloat16)


def relayout_kernel(n, sources, *refs):
    xs, (o_ref, held) = refs[:n], refs[-2:]
    me = lax.axis_index("tp")
    for i in range(o_ref.shape[0]):
        for x_ref, source in zip(xs, sources):
            held[i % 2, at(n, me, *source)] = x_ref[i]
        o_ref[i] = jnp.swapaxes(held[i % 2], 0, 1)


def relayout(n, sources, xs, whole, first, batch, block):
    count, seq_local, head_dim = xs[0].shape
    return pl.pallas_call(
        functools.partial(relayout_kernel, n, sources),
        grid=(count // block,),
        out_shape=jax.ShapeDtypeStruct((batch, seq_local, n, head_dim), xs[0].dtype),
        in_specs=[pl.BlockSpec((block, seq_local, head_dim), lambda i: (i, 0, 0))] * n
        + ([] if whole is None else [pl.BlockSpec(memory_space=pl.ANY)]),
        out_specs=pl.BlockSpec(tuple(map(pl.Element, (block, seq_local, n, head_dim))), lambda i: (first + i * block, 0, 0, 0)),
        scratch_shapes=[pltpu.VMEM((2, n, seq_local, head_dim), xs[0].dtype)],
        input_output_aliases={} if whole is None else {n: 0},
        compiler_params=ROOM,
        cost_estimate=pl.CostEstimate(flops=count * 40_000_000, bytes_accessed=4 * n * xs[0].size, transcendentals=0),
    )(*xs, *([] if whole is None else [whole]))


def last_relayout_kernel(n, sources, first, *refs):
    xs, (o_ref, held, ready, sem) = refs[:n], refs[-4:]
    me = lax.axis_index("tp")
    copies = []
    for i in range(ready.shape[0]):
        for x_ref, source in zip(xs, sources):
            held[i, at(n, me, *source)] = x_ref[i]
        ready[i] = jnp.swapaxes(held[i], 0, 1)
        copies.append(pltpu.make_async_copy(ready.at[i], o_ref.at[first + i], sem.at[i]))
        copies[-1].start()
    for copy in copies:
        copy.wait()


def last_relayout(n, sources, xs, whole, first):
    count, seq_local, head_dim = xs[0].shape
    return pl.pallas_call(
        functools.partial(last_relayout_kernel, n, sources, first),
        out_shape=jax.ShapeDtypeStruct(whole.shape, whole.dtype),
        in_specs=[pl.BlockSpec(memory_space=pltpu.VMEM)] * n + [pl.BlockSpec(memory_space=pl.ANY)],
        out_specs=pl.BlockSpec(memory_space=pl.ANY),
        scratch_shapes=[pltpu.VMEM((count, n, seq_local, head_dim), whole.dtype), pltpu.VMEM((count, seq_local, n, head_dim), whole.dtype),
                        pltpu.SemaphoreType.DMA((count,))],
        input_output_aliases={n: 0},
        compiler_params=pltpu.CompilerParams(vmem_limit_bytes=8 * 2**20),
    )(*xs, whole)


def solution(mesh):
    n = mesh.shape["tp"]
    peers = offsets(n)
    sources = [((n // 2 - h) % (n // 2), o) for h, o in peers] + [(0, False)]

    def local_step(query, k_cache, v_cache, k_new, v_new, lens):
        batch, seq_len, _, head_dim = k_cache.shape
        k_cache = k_cache.reshape(batch, seq_len, head_dim)
        v_cache = v_cache.reshape(batch, seq_len, head_dim)
        k_new = k_new.reshape(batch, head_dim)
        v_new = v_new.reshape(batch, head_dim)

        caches, news = (k_cache, v_cache), (k_new, v_new)
        own = [(0, False)]
        got = []
        for c, (a, first, count, _) in enumerate(CHUNKS):
            slabs = []
            if c == 0:
                slabs.append(pack_first(n, lens, caches[a], news[a], peers[0], count))
            slabs += pack(n, lens, caches[a], news[a], peers[len(slabs):] + own, first, count, 1, 4)
            for i, peer in enumerate(peers):
                slabs[i] = lax.ppermute(slabs[i], "tp", pairs(n, *peer))
            got.append(slabs)

        block = 8
        cache_block = pl.BlockSpec((block, seq_len, head_dim), lambda i: (i, 0, 0))
        head_block = pl.BlockSpec((block,) + query.shape[1:], lambda i: (i, 0, 0))
        vmem_spec = pl.BlockSpec(memory_space=pltpu.VMEM)
        attend = pl.pallas_call(
            attend_kernel,
            name="attend",
            grid=(batch // block,),
            out_shape=jax.ShapeDtypeStruct(query.shape, query.dtype),
            in_specs=[pl.BlockSpec(memory_space=pltpu.SMEM), head_block, cache_block, cache_block, vmem_spec, vmem_spec],
            out_specs=head_block,
            scratch_shapes=[pltpu.VMEM((batch, head_dim), jnp.float32)] * 2,
            compiler_params=ROOM,
            cost_estimate=pl.CostEstimate(flops=10**11, bytes_accessed=4 * k_cache.size, transcendentals=0),
        )
        attn = attend(lens, query, k_cache, v_cache, k_new, v_new)

        moved = [None, None]
        for c, (a, first, count, size) in enumerate(CHUNKS):
            if c + 1 < len(CHUNKS):
                moved[a] = relayout(n, sources, got[c], moved[a], first, batch, size)
            else:
                moved[a] = last_relayout(n, sources, got[c], moved[a], first)
        return attn, *moved


    head_spec = P("dp", "tp")
    entry_spec = P("dp", None, "tp")
    return jax.shard_map(local_step, mesh=mesh, in_specs=(head_spec, entry_spec, entry_spec, head_spec, head_spec, P("dp")), out_specs=(head_spec, P("dp", "tp"), P("dp", "tp")), check_vma=False)
```

```python
import functools

import jax
import jax.numpy as jnp
from jax import lax
from jax.experimental import pallas as pl
from jax.experimental.pallas import tpu as pltpu
from jax.sharding import PartitionSpec as P


MASK_VALUE = -1e30
CHUNKS = ((0, 0, 16, 16), (0, 16, 48, 24), (1, 0, 50, 25), (1, 50, 12, 6), (1, 62, 2, 2))
ROOM = pltpu.CompilerParams(vmem_limit_bytes=66_000_000)


def offsets(n):
    chips = n // 2
    far = chips // 2
    near = [h for h in range(1, chips) if h != far]
    return [(far, False), (far, True)] + [(h, False) for h in near] + [(h, True) for h in near] + [(0, True)]


def pairs(n, hops, other):
    return [(2 * c + k, 2 * ((c + hops) % (n // 2)) + ((1 - k) if other else k)) for c in range(n // 2) for k in range(2)]


def at(n, me, hops, other):
    chip = me // 2
    core = me - 2 * chip
    return 2 * lax.rem(chip + hops, n // 2) + (1 - core if other else core)


def pack_kernel(n, peers, first, pieces, lens_ref, src_ref, new_ref, *refs):
    outs, (buf, new_buf, new32, in_sem, out_sem, new_sem) = refs[:len(peers)], refs[len(peers):]
    count, seq_local = outs[0].shape[0], outs[0].shape[1]
    size = count // pieces
    me = lax.axis_index("tp")
    new_copy = pltpu.make_async_copy(new_ref, new_buf, new_sem)
    new_copy.start()
    slots = buf.shape[0]
    work = [(o, c) for o in range(len(peers)) for c in range(pieces)]

    def base(o):
        return pl.multiple_of(at(n, me, *peers[o]) * seq_local, seq_local)

    def load(w):
        o, c = work[w]
        return pltpu.make_async_copy(src_ref.at[pl.ds(first + c * size, size), pl.ds(base(o), seq_local)],
                                     buf.at[w % slots, pl.ds(0, size)], in_sem.at[w % slots])

    def store(w):
        o, c = work[w]
        return pltpu.make_async_copy(buf.at[w % slots, pl.ds(0, size)], outs[o].at[pl.ds(c * size, size)], out_sem.at[w % slots])

    ahead = slots - 1
    for w in range(min(ahead, len(work))):
        load(w).start()
    new_copy.wait()
    new32[...] = new_buf[...].astype(jnp.float32)
    positions = lax.broadcasted_iota(jnp.int32, (seq_local, 1), 0)
    for w, (o, c) in enumerate(work):
        if w + ahead < len(work):
            if w + ahead >= slots:
                store(w + ahead - slots).wait()
            load(w + ahead).start()
        load(w).wait()
        start = base(o)

        def patch(i, carry):
            b = first + c * size + i
            row = lens_ref[b] - start

            @pl.when((row >= 0) & (row < seq_local))
            def _():
                old = buf[w % slots, i]
                buf[w % slots, i] = jnp.where(positions == row, new32[pl.ds(b, 1), :].astype(old.dtype), old)

            return carry

        lax.fori_loop(0, size, patch, 0, unroll=min(size, 8))
        store(w).start()
    for w in range(max(0, len(work) - slots), len(work)):
        store(w).wait()


def pack_first_kernel(n, peer, lens_ref, src_ref, new_ref, out_ref, lens_buf, new_buf, new32, sem):
    count, seq_local = out_ref.shape[0], out_ref.shape[1]
    start = pl.multiple_of(at(n, lax.axis_index("tp"), *peer) * seq_local, seq_local)
    data = pltpu.make_async_copy(src_ref.at[pl.ds(0, count), pl.ds(start, seq_local)], out_ref, sem.at[0])
    lengths = pltpu.make_async_copy(lens_ref, lens_buf, sem.at[1])
    new = pltpu.make_async_copy(new_ref, new_buf, sem.at[2])
    for copy in (lengths, new, data):
        copy.start()
    new.wait()
    new32[...] = new_buf[...].astype(jnp.float32)
    lengths.wait()
    data.wait()
    positions = lax.broadcasted_iota(jnp.int32, (seq_local, 1), 0)
    for b in range(count):
        row = lens_buf[b] - start

        @pl.when((row >= 0) & (row < seq_local))
        def _():
            old = out_ref[b]
            out_ref[b] = jnp.where(positions == row, new32[b:b + 1, :].astype(old.dtype), old)


def pack_first(n, lens, src, new, peer, count):
    _, seq_len, head_dim = src.shape
    any_spec = pl.BlockSpec(memory_space=pl.ANY)
    return pl.pallas_call(
        functools.partial(pack_first_kernel, n, peer),
        name="pack_first",
        out_shape=pltpu.VMEM((count, seq_len // n, head_dim), src.dtype),
        in_specs=[any_spec] * 3,
        out_specs=pl.BlockSpec(memory_space=pltpu.VMEM),
        scratch_shapes=[pltpu.SMEM(lens.shape, lens.dtype), pltpu.VMEM(new.shape, new.dtype),
                        pltpu.VMEM(new.shape, jnp.float32), pltpu.SemaphoreType.DMA((3,))],
        compiler_params=ROOM,
        cost_estimate=pl.CostEstimate(flops=count * 4_000_000, bytes_accessed=4 * count * seq_len // n * head_dim, transcendentals=0),
    )(lens, src, new)


def pack(n, lens, src, new, peers, first, count, pieces, slots):
    _, seq_len, head_dim = src.shape
    seq_local = seq_len // n
    any_spec = pl.BlockSpec(memory_space=pl.ANY)
    size = count // pieces
    return pl.pallas_call(
        functools.partial(pack_kernel, n, peers, first, pieces),
        out_shape=[jax.ShapeDtypeStruct((count, seq_local, head_dim), src.dtype)] * len(peers),
        in_specs=[pl.BlockSpec(memory_space=pltpu.SMEM), any_spec, any_spec],
        out_specs=[any_spec] * len(peers),
        scratch_shapes=[pltpu.VMEM((slots, size, seq_local, head_dim), src.dtype), pltpu.VMEM(new.shape, new.dtype),
                        pltpu.VMEM(new.shape, jnp.float32), pltpu.SemaphoreType.DMA((slots,)), pltpu.SemaphoreType.DMA((slots,)), pltpu.SemaphoreType.DMA],
        compiler_params=ROOM,
        cost_estimate=pl.CostEstimate(flops=len(peers) * count * 4_000_000, bytes_accessed=4 * len(peers) * count * seq_local * head_dim, transcendentals=0),
    )(lens, src, new)


def attend_kernel(lens_ref, q_ref, k_ref, v_ref, kn_ref, vn_ref, out_ref, kn32, vn32):
    step = pl.program_id(0)
    block, seq_len, head_dim = k_ref.shape

    @pl.when(step == 0)
    def _():
        kn32[...] = kn_ref[...].astype(jnp.float32)
        vn32[...] = vn_ref[...].astype(jnp.float32)

    scale = head_dim ** -0.5
    positions = lax.broadcasted_iota(jnp.int32, (1, seq_len), 1)
    for i in range(block):
        b = step * block + i
        length = lens_ref[b]
        query = q_ref[i]
        new_k, new_v = kn32[pl.ds(b, 1), :], vn32[pl.ds(b, 1), :]
        scores = lax.dot_general(query, k_ref[i], (((1,), (1,)), ((), ())), preferred_element_type=jnp.float32)
        new_score = jnp.sum(query.astype(jnp.float32) * new_k, axis=-1, keepdims=True)
        is_new = positions == length
        scores = jnp.where(is_new, new_score, scores) * scale
        scores = jnp.where(positions <= length, scores, MASK_VALUE)
        weights = jnp.exp(scores - jnp.max(scores, axis=-1, keepdims=True))
        weights = weights / jnp.sum(weights, axis=-1, keepdims=True)
        probs = weights.astype(jnp.bfloat16)
        old = jnp.where(is_new, 0.0, weights).astype(jnp.bfloat16)
        summed = jnp.dot(old, v_ref[i], preferred_element_type=jnp.float32)
        new_prob = jnp.sum(jnp.where(is_new, probs.astype(jnp.float32), 0.0), axis=-1, keepdims=True)
        out_ref[i] = (summed + new_prob * new_v).astype(jnp.bfloat16)


def relayout_kernel(n, sources, *refs):
    xs, (o_ref, held) = refs[:n], refs[-2:]
    me = lax.axis_index("tp")
    for i in range(o_ref.shape[0]):
        for x_ref, source in zip(xs, sources):
            held[i % 2, at(n, me, *source)] = x_ref[i]
        o_ref[i] = jnp.swapaxes(held[i % 2], 0, 1)


def relayout(n, sources, xs, whole, first, batch, block):
    count, seq_local, head_dim = xs[0].shape
    return pl.pallas_call(
        functools.partial(relayout_kernel, n, sources),
        grid=(count // block,),
        out_shape=jax.ShapeDtypeStruct((batch, seq_local, n, head_dim), xs[0].dtype),
        in_specs=[pl.BlockSpec((block, seq_local, head_dim), lambda i: (i, 0, 0))] * n
        + ([] if whole is None else [pl.BlockSpec(memory_space=pl.ANY)]),
        out_specs=pl.BlockSpec(tuple(map(pl.Element, (block, seq_local, n, head_dim))), lambda i: (first + i * block, 0, 0, 0)),
        scratch_shapes=[pltpu.VMEM((2, n, seq_local, head_dim), xs[0].dtype)],
        input_output_aliases={} if whole is None else {n: 0},
        compiler_params=ROOM,
        cost_estimate=pl.CostEstimate(flops=count * 40_000_000, bytes_accessed=4 * n * xs[0].size, transcendentals=0),
    )(*xs, *([] if whole is None else [whole]))


def last_relayout_kernel(n, sources, first, *refs):
    xs, (o_ref, held, ready, sem) = refs[:n], refs[-4:]
    me = lax.axis_index("tp")
    copies = []
    for i in range(ready.shape[0]):
        for x_ref, source in zip(xs, sources):
            held[i, at(n, me, *source)] = x_ref[i]
        ready[i] = jnp.swapaxes(held[i], 0, 1)
        copies.append(pltpu.make_async_copy(ready.at[i], o_ref.at[first + i], sem.at[i]))
        copies[-1].start()
    for copy in copies:
        copy.wait()


def last_relayout(n, sources, xs, whole, first):
    count, seq_local, head_dim = xs[0].shape
    return pl.pallas_call(
        functools.partial(last_relayout_kernel, n, sources, first),
        out_shape=jax.ShapeDtypeStruct(whole.shape, whole.dtype),
        in_specs=[pl.BlockSpec(memory_space=pltpu.VMEM)] * n + [pl.BlockSpec(memory_space=pl.ANY)],
        out_specs=pl.BlockSpec(memory_space=pl.ANY),
        scratch_shapes=[pltpu.VMEM((count, n, seq_local, head_dim), whole.dtype), pltpu.VMEM((count, seq_local, n, head_dim), whole.dtype),
                        pltpu.SemaphoreType.DMA((count,))],
        input_output_aliases={n: 0},
        compiler_params=pltpu.CompilerParams(vmem_limit_bytes=8 * 2**20),
    )(*xs, whole)


def solution(mesh):
    n = mesh.shape["tp"]
    peers = offsets(n)
    sources = [((n // 2 - h) % (n // 2), o) for h, o in peers] + [(0, False)]

    def local_step(query, k_cache, v_cache, k_new, v_new, lens):
        batch, seq_len, _, head_dim = k_cache.shape
        k_cache = k_cache.reshape(batch, seq_len, head_dim)
        v_cache = v_cache.reshape(batch, seq_len, head_dim)
        k_new = k_new.reshape(batch, head_dim)
        v_new = v_new.reshape(batch, head_dim)

        caches, news = (k_cache, v_cache), (k_new, v_new)
        own = [(0, False)]
        got = []
        for c, (a, first, count, _) in enumerate(CHUNKS):
            slabs = []
            if c == 0:
                slabs.append(pack_first(n, lens, caches[a], news[a], peers[0], count))
            slabs += pack(n, lens, caches[a], news[a], peers[len(slabs):] + own, first, count, 1, 8)
            for i, peer in enumerate(peers):
                slabs[i] = lax.ppermute(slabs[i], "tp", pairs(n, *peer))
            got.append(slabs)

        block = 8
        cache_block = pl.BlockSpec((block, seq_len, head_dim), lambda i: (i, 0, 0))
        head_block = pl.BlockSpec((block,) + query.shape[1:], lambda i: (i, 0, 0))
        vmem_spec = pl.BlockSpec(memory_space=pltpu.VMEM)
        attend = pl.pallas_call(
            attend_kernel,
            name="attend",
            grid=(batch // block,),
            out_shape=jax.ShapeDtypeStruct(query.shape, query.dtype),
            in_specs=[pl.BlockSpec(memory_space=pltpu.SMEM), head_block, cache_block, cache_block, vmem_spec, vmem_spec],
            out_specs=head_block,
            scratch_shapes=[pltpu.VMEM((batch, head_dim), jnp.float32)] * 2,
            compiler_params=ROOM,
            cost_estimate=pl.CostEstimate(flops=10**11, bytes_accessed=4 * k_cache.size, transcendentals=0),
        )
        attn = attend(lens, query, k_cache, v_cache, k_new, v_new)

        moved = [None, None]
        for c, (a, first, count, size) in enumerate(CHUNKS):
            if c + 1 < len(CHUNKS):
                moved[a] = relayout(n, sources, got[c], moved[a], first, batch, size)
            else:
                moved[a] = last_relayout(n, sources, got[c], moved[a], first)
        return attn, *moved


    head_spec = P("dp", "tp")
    entry_spec = P("dp", None, "tp")
    return jax.shard_map(local_step, mesh=mesh, in_specs=(head_spec, entry_spec, entry_spec, head_spec, head_spec, P("dp")), out_specs=(head_spec, P("dp", "tp"), P("dp", "tp")), check_vma=False)
```
